128 devices in a mesh: layer: 4 (over x_lo, core), feat: 32 (over x_hi, y, z).
Axes of the slice: x: 4 (x_hi: 2, x_lo: 2; x = x_hi * 2 + x_lo), y: 4, z: 4, core: 2. Of those that a mesh axis runs over, the one named last changes fastest.
Arguments:
- inputs: bfloat16 [4, 512, 2304], P('layer', 'feat'), may hold values from -6 to 6
- targets: bfloat16 [4, 512, 2304], P('layer', 'feat'), may hold values from -64 to 64
- enc_weight: bfloat16 [4, 2304, 8192], P('layer', None, 'feat'), may hold values from -0.125 to 0.125
- enc_bias: float32 [4, 8192], P('layer', 'feat'), may hold values from -3 to 3
- dec_weight: bfloat16 [4, 4, 8192, 2304], P('layer', None, 'feat'), may hold values from -0.0625 to 0.0625
- dec_bias: float32 [4, 2304], P('layer'), may hold values from -3 to 3
Outputs:
- enc_grad: float32 [4, 2304, 8192], P('layer', None, 'feat')
- enc_bias_grad: float32 [4, 8192], P('layer', 'feat')
- dec_grad: float32 [4, 4, 8192, 2304], P('layer', None, 'feat')
- dec_bias_grad: float32 [4, 2304], P('layer')
- mean_square: float32 [], replicated
The draws below stay inside these ranges and needn't reach their ends.
All inputs are finite; a program needn't handle non-finite values.
Results may differ from the reference program's by a relative error of at most 0.0095.
Values may be sent and summed in bfloat16 or wider, within the bound.
No kernel may reach another device: no remote copies, remote signals or barrier semaphores. Data moves between devices by JAX's collectives and lax.ppermute only.
A program may use at most 128 MiB of HBM per device.

```python
import jax
import jax.numpy as jnp

D = 2304
F = 8192
MB = 128
LAYERS = 4
TOKENS = 512


def draw_targets(key, part):
    key_base = jax.random.fold_in(key, 11)
    base = jnp.clip(jax.random.normal(key_base, (LAYERS, TOKENS, D), jnp.float32), -5.0, 5.0)
    order = (jnp.arange(LAYERS)[:, None] * TOKENS + jnp.arange(TOKENS)[None, :]).astype(jnp.float32)
    rising = 1.0 + 2.0 * order / (LAYERS * TOKENS - 1.0)
    values = base
    values = jnp.clip(values * rising[:, :, None], -64.0, 64.0)
    return values.astype(jnp.bfloat16)


def steps_of(key, dims, pieces, least, top_value):
    factor_of, own = 1.0, jax.random.fold_in(key, 6)
    for position, parts in pieces:
        draws = jnp.exp(jax.random.uniform(jax.random.fold_in(own, position), (parts,), jnp.float32, least / len(pieces), top_value / len(pieces)))
        factor_of = factor_of * jnp.repeat(draws, dims[position] // parts).reshape([-1 if axis == position else 1 for axis in range(len(dims))])
    return factor_of


def bell_draw(own_key, shape, width, most, cuts=(), kind=jnp.bfloat16):
    values = jax.random.normal(own_key, shape, jnp.float32) * width
    if len(cuts) > 0:
        values = steps_of(own_key, shape, cuts, -0.22, 0.18) * values
    return jnp.clip(values, min=-most, max=most).astype(kind)


def setup_inputs(seed: int = 0) -> dict:
    key_of = jax.random.split(jax.random.key(seed), 7)
    inputs = bell_draw(key_of[0], (LAYERS, TOKENS, D), 1.0, 6.0, ((0, 4), (1, 32)))
    targets = draw_targets(jax.random.fold_in(key_of[6], 71), 0)
    enc_weight = bell_draw(key_of[2], (LAYERS, D, F), D ** -0.5, 0.125, ((0, 4), (2, 32)))
    enc_bias = bell_draw(key_of[3], (LAYERS, F), 0.5, 3.0, ((0, 4), (1, 32)), jnp.float32)
    dec_weight = bell_draw(key_of[4], (LAYERS, LAYERS, F, D), F ** -0.5, 0.0625, ((0, 4), (2, 32)))
    dec_bias = bell_draw(key_of[5], (LAYERS, D), 0.5, 3.0, ((0, 4),), jnp.float32)
    return {"inputs": inputs, "targets": targets, "enc_weight": enc_weight, "enc_bias": enc_bias, "dec_weight": dec_weight, "dec_bias": dec_bias}


def reference(inputs, targets, enc_weight, enc_bias, dec_weight, dec_bias):
    depth = inputs.shape[0]
    tok_count = inputs.shape[1]
    model_width = inputs.shape[2]
    pre_list = []
    act_list = []
    for source in range(depth):
        pre_act = jnp.dot(inputs[source], enc_weight[source], preferred_element_type=jnp.float32) + enc_bias[source]
        pre_list.append(pre_act)
        act_list.append(jnp.maximum(pre_act, 0.0).astype(jnp.bfloat16))
    residual_list = []
    squares = jnp.zeros((), jnp.float32)
    bias_rows = []
    for target in range(depth):
        rebuilt = jnp.zeros((tok_count, model_width), jnp.float32) + dec_bias[target]
        for source in range(target + 1):
            rebuilt = rebuilt + jnp.dot(act_list[source], dec_weight[source, target], preferred_element_type=jnp.float32)
        residual = rebuilt - targets[target].astype(jnp.float32)
        squares = squares + jnp.sum(residual * residual)
        bias_rows.append(jnp.sum(residual, axis=0) / MB)
        residual_list.append(residual.astype(jnp.bfloat16))
    mean_square = squares / (depth * tok_count * model_width)
    dec_bias_grad = jnp.stack(bias_rows)
    dec_rows = []
    enc_rows = []
    enc_bias_rows = []
    for source in range(depth):
        slots = []
        grad_act = jnp.zeros(pre_list[source].shape, jnp.float32)
        for target in range(depth):
            if target >= source:
                slots.append(jnp.dot(act_list[source].T, residual_list[target], preferred_element_type=jnp.float32) / MB)
                grad_act = grad_act + jnp.dot(residual_list[target], dec_weight[source, target].T, preferred_element_type=jnp.float32)
            else:
                slots.append(jnp.zeros((dec_weight.shape[2], model_width), jnp.float32))
        dec_rows.append(jnp.stack(slots))
        grad_act = grad_act / MB
        grad_pre = jnp.where(pre_list[source] > 0, grad_act, 0.0)
        enc_bias_rows.append(jnp.sum(grad_pre, axis=0))
        enc_rows.append(jnp.dot(inputs[source].T, grad_pre.astype(jnp.bfloat16), preferred_element_type=jnp.float32))
    return jnp.stack(enc_rows), jnp.stack(enc_bias_rows), jnp.stack(dec_rows), dec_bias_grad, mean_square
```

```python
import jax
import jax.numpy as jnp
from jax import lax
from jax.sharding import Mesh, PartitionSpec as P

MB = 128
AXES = ("x_lo", "core", "x_hi", "y", "z")
SIZES = (2, 2, 2, 4, 4)
LAYER = ("x_lo", "core")
FEAT = ("x_hi", "y", "z")


def ring(axis, step):
    return axis, [(i, (i + step) % 4) for i in range(4)]


def ring_even(axis, step):
    return ("x_lo", axis), [(i, (i + step) % 4) for i in range(4)]


def move(value, route):
    axis, pairs = route
    return lax.ppermute(value, axis, pairs)


def swap(value, axis):
    return lax.ppermute(value, axis, [(0, 1), (1, 0)])


def gather4(value, axis, route):
    return [value] + [move(value, route(axis, -k)) for k in (1, 2, 3)]


def scatter4(blocks, axis, route):
    arrived = [move(blocks[k], route(axis, k)) for k in (2, 1, 3)]
    total = blocks[0].astype(jnp.float32)
    for piece in arrived:
        total = total + piece.astype(jnp.float32)
    return total


EVEN_TO_ODD = [[(0, 2), (1, 3)], [(0, 3), (1, 2)]]
ODD_TO_EVEN = [[(2, 0), (3, 1)], [(2, 1), (3, 0)]]


def body(inputs, targets, enc_weight, enc_bias, dec_weight, dec_bias):
    x_lo = lax.axis_index("x_lo")
    core = lax.axis_index("core")
    layer = 2 * x_lo + core
    features = enc_weight.shape[2]
    rows, width = inputs.shape[1:]
    tokens = 32 * rows
    half = width // 2
    bf16, f32 = jnp.bfloat16, jnp.float32

    pairs = dec_weight[0].reshape(2, 2, features, width)
    keep = lax.dynamic_index_in_dim(pairs, core, 1, keepdims=False)
    give = lax.dynamic_index_in_dim(pairs, 1 - core, 1, keepdims=False)
    got = swap(give, "core")
    slot_target = 2 * jnp.arange(2) + core
    own_valid = (slot_target >= layer).astype(bf16)[:, None, None]
    pair_valid = (slot_target >= layer + 1 - 2 * core).astype(bf16)[:, None, None]
    weight = jnp.concatenate([keep * own_valid, got * pair_valid], axis=1)

    both = jnp.stack([inputs[0], swap(inputs[0], "x_hi")])
    lo = jnp.stack(gather4(both[:, :, :half], "z", ring))
    lo = jnp.stack(gather4(lo, "y", ring))
    hi = jnp.stack(gather4(both[:, :, half:], "y", ring))
    hi = jnp.stack(gather4(hi, "z", ring), axis=1)
    lo = lo.reshape(tokens, half)
    hi = hi.reshape(tokens, half)
    pre_act = (
        jnp.dot(lo, enc_weight[0, :half], preferred_element_type=f32)
        + jnp.dot(hi, enc_weight[0, half:], preferred_element_type=f32)
        + enc_bias[0]
    )
    activity = jnp.maximum(pre_act, 0.0).astype(bf16)
    act_pair = jnp.concatenate([activity, swap(activity, "core")], axis=1)

    def turned(value):
        shape = value.shape
        return value.reshape(4, 4, shape[0] // 16, *shape[1:]).swapaxes(0, 1).reshape(shape)

    act_of = [act_pair, turned(act_pair)]
    routes = [("y", "z", ring_even), ("z", "y", ring)]
    held = []
    for slot in range(2):
        first, second, route = routes[slot]
        blocks = act_of[slot].reshape(4, tokens // 4, 2 * features)
        partial = [None] * 4
        for k in (2, 1, 3, 0):
            partial[k] = jnp.dot(blocks[k], weight[slot], preferred_element_type=f32).astype(bf16)
        total = scatter4(partial, first, route).astype(bf16)
        total = total.reshape(4, 2, rows, width)
        held.append(scatter4([total[k] for k in range(4)], second, route).astype(bf16))

    chips = ("x_lo", "x_hi")
    own = jnp.where(x_lo == 0, held[0], held[1])
    summed = own[0].astype(f32) + swap(own[1], "x_hi").astype(f32)
    for other in range(2):
        summed = summed + lax.ppermute(held[1][other], chips, EVEN_TO_ODD[other]).astype(f32)
    residual = summed + dec_bias[0] - targets[0].astype(f32)
    error = residual.astype(bf16)

    here = jnp.stack([error, swap(error, "x_hi")])
    there = jnp.stack([lax.ppermute(error, chips, ODD_TO_EVEN[other]) for other in range(2)])
    start = [here, jnp.where(x_lo == 0, there, here)]
    errors, pair_errors = [], []
    for slot in range(2):
        first, second, route = routes[slot]
        plane = jnp.stack(gather4(start[slot], second, route))
        pieces = gather4(plane.reshape(tokens // 4, width), first, route)
        errors.append(jnp.concatenate(pieces))
        pair_errors.append(jnp.concatenate([swap(piece, "core") for piece in pieces]))

    back = [
        lax.dot_general(errors[s], weight[s], (((1,), (1,)), ((), ())), preferred_element_type=f32)
        for s in range(2)
    ]
    back = back[0] + turned(back[1])
    grad_act = (back[:, :features] + swap(back[:, features:], "core")) / MB
    grad_pre = jnp.where(pre_act > 0, grad_act, 0.0)
    enc_bias_grad = jnp.sum(grad_pre, axis=0)[None]
    grad_pre_b = grad_pre.astype(bf16)
    enc_grad = jnp.concatenate(
        [
            lax.dot_general(part, grad_pre_b, (((0,), (0,)), ((), ())), preferred_element_type=f32)
            for part in (lo, hi)
        ]
    )[None]

    acts = [activity, turned(activity)]
    slots = []
    for target in range(4):
        slot, parity = target // 2, target % 2
        err = jnp.where(core == parity, errors[slot], pair_errors[slot])
        grad = lax.dot_general(acts[slot], err, (((0,), (0,)), ((), ())), preferred_element_type=f32)
        slots.append(jnp.where(target >= layer, grad / MB, 0.0))
    dec_grad = jnp.stack(slots)[None]

    mine = jnp.where(x_lo == 0, errors[0], errors[1]).astype(f32)
    dec_bias_grad = (jnp.sum(mine, axis=0) / MB)[None]
    squares = jnp.zeros((), f32)
    for slot in range(2):
        wide = errors[slot].astype(f32)
        squares = squares + jnp.sum(wide * wide)
    squares = jnp.broadcast_to(squares, (8, 128))
    squares = squares + swap(squares, "core")
    sent = lax.ppermute(squares, "x_lo", [(0, 1)])
    squares = jnp.where(x_lo == 0, squares, sent)[0, 0]
    mean_square = squares / (4 * tokens * width)
    return (enc_grad, enc_bias_grad, dec_grad, dec_bias_grad, mean_square)


def solution(mesh):
    fine = Mesh(mesh.devices.reshape(SIZES), AXES)
    placed = (
        P(LAYER, FEAT, None),
        P(LAYER, FEAT, None),
        P(LAYER, None, FEAT),
        P(LAYER, FEAT),
        P(LAYER, None, FEAT, None),
        P(LAYER, None),
    )
    return jax.shard_map(
        body,
        mesh=fine,
        in_specs=placed,
        out_specs=(
            P(LAYER, None, FEAT),
            P(LAYER, FEAT),
            P(LAYER, None, FEAT, None),
            P(LAYER, None),
            P(),
        ),
        check_vma=False,
    )
```

```python
import jax
import jax.numpy as jnp
from jax import lax
from jax.sharding import Mesh, PartitionSpec as P

MB = 128
AXES = ("x_lo", "core", "x_hi", "y", "z")
SIZES = (2, 2, 2, 4, 4)
LAYER = ("x_lo", "core")
FEAT = ("x_hi", "y", "z")
bf16, f32 = jnp.bfloat16, jnp.float32


PLANE = ("core", "y", "z")


def route(ring, step):
    pairs = []
    for device in range(32):
        core, y, z = device // 16, device // 4 % 4, device % 4
        if (ring == "u") == (core == 0):
            to = core * 16 + (y + step) % 4 * 4 + z
        else:
            to = core * 16 + y * 4 + (z + step) % 4
        pairs.append((device, to))
    return pairs


def move(value, ring, step):
    return lax.ppermute(value, PLANE, route(ring, step))


def swap(value, axis):
    return lax.ppermute(value, axis, [(0, 1), (1, 0)])


def gather4(value, ring):
    far, up, down = move(value, ring, 2), move(value, ring, -1), move(value, ring, 1)
    return [value, up, far, down]


def scatter4(blocks, ring):
    total = blocks[0].astype(f32)
    for piece in [move(blocks[k], ring, k) for k in (2, 1, 3)]:
        total = total + piece.astype(f32)
    return total


def relay4(value, ring):
    up, down = move(value, ring, -1), move(value, ring, 1)
    half = value.shape[0] // 2
    far = jnp.concatenate([move(up[:half], ring, -1), move(down[half:], ring, 1)])
    return [value, up, far, down]


ACROSS = [(0, 3), (1, 2), (2, 1), (3, 0)]


def turned(value):
    shape = value.shape
    return value.reshape(4, 4, shape[0] // 16, *shape[1:]).swapaxes(0, 1).reshape(shape)


def body(inputs, targets, enc_weight, enc_bias, dec_weight, dec_bias):
    x_lo = lax.axis_index("x_lo")
    core = lax.axis_index("core")
    layer = 2 * x_lo + core
    features = enc_weight.shape[2]
    rows, width = inputs.shape[1:]
    tokens = 32 * rows

    both = jnp.concatenate([inputs[0], swap(inputs[0], "x_hi")])
    column = jnp.concatenate(gather4(both, "v"))
    both, dec_weight = lax.optimization_barrier((both, dec_weight))
    tokens_in = jnp.concatenate(relay4(column, "u"))

    pairs = dec_weight[0].reshape(2, 2, features, width)
    keep = lax.dynamic_index_in_dim(pairs, core, 1, keepdims=False)
    give = lax.dynamic_index_in_dim(pairs, 1 - core, 1, keepdims=False)
    got = swap(give, "core")
    slot = 2 * jnp.arange(2, dtype=jnp.int32)
    own_valid = (slot + core >= layer).astype(bf16)[:, None, None]
    pair_valid = (slot + core >= layer + 1 - 2 * core).astype(bf16)[:, None, None]
    weight = jnp.concatenate([keep * own_valid, got * pair_valid], axis=1)

    pre_act = jnp.dot(tokens_in, enc_weight[0], preferred_element_type=f32) + enc_bias[0]
    activity = jnp.maximum(pre_act, 0.0).astype(bf16)
    act_pair = jnp.concatenate([activity, turned(swap(activity, "core"))], axis=1)

    blocks = act_pair.reshape(4, tokens // 4, 2 * features)
    partial = [None] * 4
    for k in (2, 1, 3, 0):
        partial[k] = jnp.einsum(
            "tf,sfd->std", blocks[k], weight, preferred_element_type=f32
        ).astype(bf16)
    total = scatter4(partial, "u").astype(bf16).reshape(2, 4, 2 * rows, width)
    total = scatter4([total[:, k] for k in range(4)], "v").reshape(2, 2, rows, width)

    shift = dec_bias[0] - targets[0].astype(f32)
    owner = (jnp.arange(2) == x_lo).astype(f32)[:, None, None]
    total = jnp.stack([total[:, 0] + owner * shift, total[:, 1]], axis=1)
    terms = total.astype(bf16)
    partner = swap(terms, "x_hi")
    same = swap(terms[1], "x_lo")
    other = lax.ppermute(terms[1], ("x_lo", "x_hi"), ACROSS)
    residual = terms.astype(f32) + partner[:, ::-1].astype(f32)
    second = residual[1] + same.astype(f32) + other[::-1].astype(f32)
    error = jnp.stack([residual[0], second]).astype(bf16).reshape(2, 2 * rows, width)
    column = jnp.concatenate(
        [piece[:, None] for piece in gather4(error, "v")], axis=1
    )
    mine = relay4(column.reshape(2, tokens // 4, width), "u")
    pair = [swap(piece, "core") for piece in mine]

    def back(piece, slot):
        return lax.dot_general(
            piece[slot], weight[slot], (((1,), (1,)), ((), ())), preferred_element_type=f32
        )

    grad_both = jnp.concatenate([back(piece, 0) + back(piece, 1) for piece in mine])
    grad_act = (grad_both[:, :features] + turned(swap(grad_both[:, features:], "core"))) / MB
    grad_pre = jnp.where(pre_act > 0, grad_act, 0.0)
    enc_bias_grad = jnp.sum(grad_pre, axis=0)[None]
    enc_grad = lax.dot_general(
        tokens_in,
        grad_pre.astype(bf16),
        (((0,), (0,)), ((), ())),
        preferred_element_type=f32,
    )[None]

    errors = [[jnp.concatenate([p[k] for p in held]) for k in range(2)] for held in (mine, pair)]
    orders = (activity, turned(activity))
    slots = []
    for target in range(4):
        parity = core == target % 2
        err = jnp.where(parity, errors[0][target // 2], errors[1][target // 2])
        act = jnp.where(parity, *orders)
        grad = lax.dot_general(act, err, (((0,), (0,)), ((), ())), preferred_element_type=f32)
        slots.append(jnp.where(target >= layer, grad / MB, 0.0))
    dec_grad = jnp.stack(slots)

    ones = jnp.ones((8, tokens // 4), bf16)
    same_row = jnp.eye(tokens // 4, dtype=f32)
    sums, grams = 0.0, 0.0
    for piece in mine:
        sums = sums + jnp.einsum("rt,std->srd", ones, piece, preferred_element_type=f32)
        grams = grams + jnp.einsum("std,sud->stu", piece, piece, preferred_element_type=f32)
    sums = lax.dynamic_index_in_dim(sums, x_lo, 0, keepdims=False)[0]
    squares = jnp.sum(grams * same_row)
    dec_bias_grad = (sums / MB)[None]
    square = jnp.broadcast_to(squares, (8, 128))
    square = square + swap(square, "core")
    square = jnp.where(x_lo == 0, square, lax.ppermute(square, "x_lo", [(0, 1)]))
    mean_square = square[0, 0] / (4 * tokens * width)
    return (enc_grad, enc_bias_grad, dec_grad[None], dec_bias_grad, mean_square)


def solution(mesh):
    fine = Mesh(mesh.devices.reshape(SIZES), AXES)
    placed = (
        P(LAYER, FEAT, None),
        P(LAYER, FEAT, None),
        P(LAYER, None, FEAT),
        P(LAYER, FEAT),
        P(LAYER, None, FEAT, None),
        P(LAYER, None),
    )
    return jax.shard_map(
        body,
        mesh=fine,
        in_specs=placed,
        out_specs=(
            P(LAYER, None, FEAT),
            P(LAYER, FEAT),
            P(LAYER, None, FEAT, None),
            P(LAYER, None),
            P(),
        ),
        check_vma=False,
    )
```

```python
import jax
import jax.numpy as jnp
from jax import lax
from jax.experimental.layout import Layout, with_layout_constraint
from jax.sharding import Mesh, PartitionSpec as P


MB = 128
ROW_MAJOR = Layout(major_to_minor=(0, 1, 2))
AXES = ("x_lo", "core", "x_hi", "y", "z")
SIZES = (2, 2, 2, 4, 4)
LAYER = ("x_lo", "core")
FEAT = ("x_hi", "y", "z")
bf16, f32 = jnp.bfloat16, jnp.float32


PLANE = ("core", "y", "z")


def route(ring, step):
    pairs = []
    for device in range(32):
        core, y, z = device // 16, device // 4 % 4, device % 4
        if (ring == "u") == (core == 0):
            to = core * 16 + (y + step) % 4 * 4 + z
        else:
            to = core * 16 + y * 4 + (z + step) % 4
        pairs.append((device, to))
    return pairs


def move(value, ring, step):
    return lax.ppermute(value, PLANE, route(ring, step))


def swap(value, axis):
    return lax.ppermute(value, axis, [(0, 1), (1, 0)])


def gather4(value, ring):
    far, up, down = move(value, ring, 2), move(value, ring, -1), move(value, ring, 1)
    return [value, up, far, down]


def scatter4(blocks, ring):
    arrived = []
    for k in (2, 1, 3):
        arrived.append(move(blocks[k], ring, k))
    total = blocks[0].astype(f32)
    for piece in arrived:
        total = total + piece.astype(f32)
    return total


def relay4(value, ring):
    up, down = move(value, ring, -1), move(value, ring, 1)
    half = value.shape[0] // 2
    far = jnp.concatenate([move(up[:half], ring, -1), move(down[half:], ring, 1)])
    return [value, up, far, down]


ACROSS = [(0, 3), (1, 2), (2, 1), (3, 0)]


def turned(value):
    shape = value.shape
    return value.reshape(4, 4, shape[0] // 16, *shape[1:]).swapaxes(0, 1).reshape(shape)


def body(inputs, targets, enc_weight, enc_bias, dec_weight, dec_bias):
    x_lo = lax.axis_index("x_lo")
    core = lax.axis_index("core")
    layer = 2 * x_lo + core
    features = enc_weight.shape[2]
    rows, width = inputs.shape[1:]
    tokens = 32 * rows

    both = jnp.concatenate([inputs[0], swap(inputs[0], "x_hi")])
    column = jnp.concatenate(gather4(both, "v"))
    both, dec_weight = lax.optimization_barrier((both, dec_weight))
    tokens_in = jnp.concatenate(relay4(column, "u"))

    pairs = dec_weight[0].reshape(2, 2, features, width)
    keep = lax.dynamic_index_in_dim(pairs, core, 1, keepdims=False)
    give = lax.dynamic_index_in_dim(pairs, 1 - core, 1, keepdims=False)
    got = swap(give, "core")
    slot = 2 * jnp.arange(2, dtype=jnp.int32)
    own_valid = (slot + core >= layer).astype(bf16)[:, None, None]
    pair_valid = (slot + core >= layer + 1 - 2 * core).astype(bf16)[:, None, None]
    weight = jnp.concatenate([keep * own_valid, got * pair_valid], axis=1)

    pre_act = jnp.dot(tokens_in, enc_weight[0], preferred_element_type=f32) + enc_bias[0]
    activity = jnp.maximum(pre_act, 0.0).astype(bf16)
    act_pair = jnp.concatenate([activity, turned(swap(activity, "core"))], axis=1)

    blocks = act_pair.reshape(4, tokens // 4, 2 * features)
    partial = [None] * 4
    for k in (2, 1, 3, 0):
        partial[k] = jnp.einsum(
            "tf,sfd->std", blocks[k], weight, preferred_element_type=f32
        ).astype(bf16)

    partial[0] = lax.optimization_barrier(with_layout_constraint(partial[0], ROW_MAJOR))
    total = scatter4(partial, "u").astype(bf16).reshape(2, 4, 2 * rows, width)
    total = scatter4([total[:, k] for k in range(4)], "v").reshape(2, 2, rows, width)

    shift = dec_bias[0] - targets[0].astype(f32)
    owner = (jnp.arange(2) == x_lo).astype(f32)[:, None, None]
    total = jnp.stack([total[:, 0] + owner * shift, total[:, 1]], axis=1)
    terms = total.astype(bf16)
    partner = swap(terms, "x_hi")
    same = swap(terms[1], "x_lo")
    other = lax.ppermute(terms[1], ("x_lo", "x_hi"), ACROSS)
    residual = terms.astype(f32) + partner[:, ::-1].astype(f32)
    second = residual[1] + same.astype(f32) + other[::-1].astype(f32)
    error = jnp.stack([residual[0], second]).astype(bf16).reshape(2, 2 * rows, width)
    column = jnp.concatenate(
        [piece[:, None] for piece in gather4(error, "v")], axis=1
    )
    mine = relay4(column.reshape(2, tokens // 4, width), "u")
    pair = [swap(piece, "core") for piece in mine]

    def back(piece, slot):
        return lax.dot_general(
            piece[slot], weight[slot], (((1,), (1,)), ((), ())), preferred_element_type=f32
        )

    grad_both = jnp.concatenate([back(piece, 0) + back(piece, 1) for piece in mine])
    grad_act = (grad_both[:, :features] + turned(swap(grad_both[:, features:], "core"))) / MB
    grad_pre = jnp.where(pre_act > 0, grad_act, 0.0)
    enc_bias_grad = jnp.sum(grad_pre, axis=0)[None]
    enc_grad = lax.dot_general(
        tokens_in,
        grad_pre.astype(bf16),
        (((0,), (0,)), ((), ())),
        preferred_element_type=f32,
    )[None]

    errors = [[jnp.concatenate([p[k] for p in held]) for k in range(2)] for held in (mine, pair)]
    orders = (activity, turned(activity))
    slots = []
    for target in range(4):
        parity = core == target % 2
        err = jnp.where(parity, errors[0][target // 2], errors[1][target // 2])
        act = jnp.where(parity, *orders)
        grad = lax.dot_general(act, err, (((0,), (0,)), ((), ())), preferred_element_type=f32)
        slots.append(jnp.where(target >= layer, grad / MB, 0.0))
    dec_grad = jnp.stack(slots)

    ones = jnp.ones((8, tokens // 4), bf16)
    same_row = jnp.eye(tokens // 4, dtype=f32)
    sums, grams = 0.0, 0.0
    for piece in mine:
        sums = sums + jnp.einsum("rt,std->srd", ones, piece, preferred_element_type=f32)
        grams = grams + jnp.einsum("std,sud->stu", piece, piece, preferred_element_type=f32)
    sums = lax.dynamic_index_in_dim(sums, x_lo, 0, keepdims=False)[0]
    squares = jnp.sum(grams * same_row)
    dec_bias_grad = (sums / MB)[None]
    square = jnp.broadcast_to(squares, (8, 128))
    square = square + swap(square, "core")
    square = jnp.where(x_lo == 0, square, lax.ppermute(square, "x_lo", [(0, 1)]))
    mean_square = square[0, 0] / (4 * tokens * width)
    return (enc_grad, enc_bias_grad, dec_grad[None], dec_bias_grad, mean_square)


def solution(mesh):
    fine = Mesh(mesh.devices.reshape(SIZES), AXES)
    placed = (
        P(LAYER, FEAT, None),
        P(LAYER, FEAT, None),
        P(LAYER, None, FEAT),
        P(LAYER, FEAT),
        P(LAYER, None, FEAT, None),
        P(LAYER, None),
    )
    return jax.shard_map(
        body,
        mesh=fine,
        in_specs=placed,
        out_specs=(
            P(LAYER, None, FEAT),
            P(LAYER, FEAT),
            P(LAYER, None, FEAT, None),
            P(LAYER, None),
            P(),
        ),
        check_vma=False,
    )
```

```python
import jax
import jax.numpy as jnp
from jax import lax
from jax.experimental.layout import Layout, with_layout_constraint
from jax.sharding import Mesh, PartitionSpec as P


MB = 128
ROW_MAJOR = Layout(major_to_minor=(0, 1, 2))
AXES = ("x_lo", "core", "x_hi", "y", "z")
SIZES = (2, 2, 2, 4, 4)
LAYER = ("x_lo", "core")
FEAT = ("x_hi", "y", "z")
bf16, f32 = jnp.bfloat16, jnp.float32


PLANE = ("core", "y", "z")


def route(ring, step):
    pairs = []
    for device in range(32):
        core, y, z = device // 16, device // 4 % 4, device % 4
        if (ring == "u") == (core == 0):
            to = core * 16 + (y + step) % 4 * 4 + z
        else:
            to = core * 16 + y * 4 + (z + step) % 4
        pairs.append((device, to))
    return pairs


def move(value, ring, step):
    return lax.ppermute(value, PLANE, route(ring, step))


def swap(value, axis):
    return lax.ppermute(value, axis, [(0, 1), (1, 0)])


def gather4(value, ring):
    far, up, down = move(value, ring, 2), move(value, ring, -1), move(value, ring, 1)
    return [value, up, far, down]


def scatter4(blocks, ring):
    arrived = []
    for k in (2, 1, 3):
        arrived.append(move(blocks[k], ring, k))
    return [blocks[0], *arrived]


def summed(pieces):
    total = pieces[0].astype(f32)
    for piece in pieces[1:]:
        total = total + piece.astype(f32)
    return total


def relay4(value, ring):
    up, down = move(value, ring, -1), move(value, ring, 1)
    half = value.shape[0] // 2
    far = jnp.concatenate([move(up[:half], ring, -1), move(down[half:], ring, 1)])
    return [value, up, far, down]


ACROSS = [(0, 3), (1, 2), (2, 1), (3, 0)]


def turned(value):
    shape = value.shape
    return value.reshape(4, 4, shape[0] // 16, *shape[1:]).swapaxes(0, 1).reshape(shape)


def body(inputs, targets, enc_weight, enc_bias, dec_weight, dec_bias):
    x_lo = lax.axis_index("x_lo")
    core = lax.axis_index("core")
    layer = 2 * x_lo + core
    features = enc_weight.shape[2]
    rows, width = inputs.shape[1:]
    tokens = 32 * rows

    both = jnp.concatenate([inputs[0], swap(inputs[0], "x_hi")])
    column = jnp.concatenate(gather4(both, "v"))
    both, dec_weight = lax.optimization_barrier((both, dec_weight))
    tokens_in = jnp.concatenate(relay4(column, "u"))

    pairs = dec_weight[0].reshape(2, 2, features, width)
    keep = lax.dynamic_index_in_dim(pairs, core, 1, keepdims=False)
    give = lax.dynamic_index_in_dim(pairs, 1 - core, 1, keepdims=False)
    got = swap(give, "core")
    slot = 2 * jnp.arange(2, dtype=jnp.int32)
    own_valid = (slot + core >= layer).astype(bf16)[:, None, None]
    pair_valid = (slot + core >= layer + 1 - 2 * core).astype(bf16)[:, None, None]
    weight = jnp.concatenate([keep * own_valid, got * pair_valid], axis=1)
    weight = lax.optimization_barrier(with_layout_constraint(weight, ROW_MAJOR))

    pre_act = jnp.dot(tokens_in, enc_weight[0], preferred_element_type=f32) + enc_bias[0]
    activity = jnp.maximum(pre_act, 0.0).astype(bf16)
    act_pair = jnp.concatenate([activity, turned(swap(activity, "core"))], axis=1)

    blocks = act_pair.reshape(4, tokens // 4, 2 * features)
    partial = [None] * 4
    for k in (2, 1, 3, 0):
        partial[k] = jnp.einsum(
            "tf,sfd->std", blocks[k], weight, preferred_element_type=f32
        ).astype(bf16)
        partial[k] = with_layout_constraint(partial[k], ROW_MAJOR)

    partial[0] = lax.optimization_barrier(partial[0])
    pieces = [p.reshape(2, 4, 2 * rows, width) for p in scatter4(partial, "u")]
    blocks = [summed([p[:, k] for p in pieces]).astype(bf16) for k in range(4)]
    total = summed(scatter4(blocks, "v")).reshape(2, 2, rows, width)

    shift = dec_bias[0] - targets[0].astype(f32)
    owner = (jnp.arange(2) == x_lo).astype(f32)[:, None, None]
    total = jnp.stack([total[:, 0] + owner * shift, total[:, 1]], axis=1)
    terms = total.astype(bf16)
    partner = swap(terms, "x_hi")
    same = swap(terms[1], "x_lo")
    other = lax.ppermute(terms[1], ("x_lo", "x_hi"), ACROSS)
    residual = terms.astype(f32) + partner[:, ::-1].astype(f32)
    second = residual[1] + same.astype(f32) + other[::-1].astype(f32)
    error = jnp.stack([residual[0], second]).astype(bf16).reshape(2, 2 * rows, width)
    column = jnp.concatenate(
        [piece[:, None] for piece in gather4(error, "v")], axis=1
    )
    mine = relay4(column.reshape(2, tokens // 4, width), "u")
    pair = [swap(piece, "core") for piece in mine]

    def back(piece, slot):
        return lax.dot_general(
            piece[slot], weight[slot], (((1,), (1,)), ((), ())), preferred_element_type=f32
        )

    grad_both = jnp.concatenate([back(piece, 0) + back(piece, 1) for piece in mine])
    grad_act = (grad_both[:, :features] + turned(swap(grad_both[:, features:], "core"))) / MB
    grad_pre = jnp.where(pre_act > 0, grad_act, 0.0)
    enc_bias_grad = jnp.sum(grad_pre, axis=0)[None]
    enc_grad = lax.dot_general(
        tokens_in,
        grad_pre.astype(bf16),
        (((0,), (0,)), ((), ())),
        preferred_element_type=f32,
    )[None]

    errors = [[jnp.concatenate([p[k] for p in held]) for k in range(2)] for held in (mine, pair)]
    products = [
        [
            lax.dot_general(act, err, (((0,), (0,)), ((), ())), preferred_element_type=f32)
            for err in errs
        ]
        for act, errs in zip((activity, turned(activity)), errors)
    ]
    slots = []
    for target in range(4):
        grad = jnp.where(core == target % 2, *[p[target // 2] for p in products])
        slots.append(jnp.where(target >= layer, grad / MB, 0.0))
    dec_grad = jnp.stack(slots)

    ones = jnp.ones((8, tokens // 4), bf16)
    same_row = jnp.eye(tokens // 4, dtype=f32)
    sums, grams = 0.0, 0.0
    for piece in mine:
        sums = sums + jnp.einsum("rt,std->srd", ones, piece, preferred_element_type=f32)
        grams = grams + jnp.einsum("std,sud->stu", piece, piece, preferred_element_type=f32)
    sums = lax.dynamic_index_in_dim(sums, x_lo, 0, keepdims=False)[0]
    squares = jnp.sum(grams * same_row)
    dec_bias_grad = (sums / MB)[None]
    square = jnp.broadcast_to(squares, (8, 128))
    square = square + swap(square, "core")
    square = jnp.where(x_lo == 0, square, lax.ppermute(square, "x_lo", [(0, 1)]))
    mean_square = square[0, 0] / (4 * tokens * width)
    return (enc_grad, enc_bias_grad, dec_grad[None], dec_bias_grad, mean_square)


def solution(mesh):
    fine = Mesh(mesh.devices.reshape(SIZES), AXES)
    placed = (
        P(LAYER, FEAT, None),
        P(LAYER, FEAT, None),
        P(LAYER, None, FEAT),
        P(LAYER, FEAT),
        P(LAYER, None, FEAT, None),
        P(LAYER, None),
    )
    return jax.shard_map(
        body,
        mesh=fine,
        in_specs=placed,
        out_specs=(
            P(LAYER, None, FEAT),
            P(LAYER, FEAT),
            P(LAYER, None, FEAT, None),
            P(LAYER, None),
            P(),
        ),
        check_vma=False,
    )
```
